256 devices in a mesh: obs: 64 (over z, y_hi, x), chan: 4 (over y_lo, core).
Axes of the slice: x: 4, y: 4 (y_hi: 2, y_lo: 2; y = y_hi * 2 + y_lo), z: 8, core: 2. Of those that a mesh axis runs over, the one named last changes fastest.
Arguments:
- departures: bfloat16 [8192, 131072], P('chan', 'obs'), may hold values from -8 to 8
- predictors: bfloat16 [10, 131072], P(None, 'obs'), may hold values from -3 to 3
- inv_band: bfloat16 [63, 8192], P(None, 'chan'), may hold values from -1 to 2.5
- band_id: int32 [8192], replicated, may hold values from 0 to 340, never falling along the last dimension, each value on 1 to 32 neighbouring positions
- line_counts: int32 [1024], P('obs'), may hold values from 24 to 128
Outputs:
- gram: float32 [100, 8192], P(None, ('chan', 'obs'))
- rhs: float32 [10, 8192], P(None, ('chan', 'obs'))
The draws below stay inside these ranges and needn't reach their ends.
Inputs may be any that keep to these rules, and one draw needn't show every extreme that they name: `band_id`: band numbers never fall along the channels; a band spans 1 to 32 channels. `line_counts`: slots of a scan line at or beyond its count are empty.
All inputs are finite; a program needn't handle non-finite values.
Results may differ from the reference program's by a relative error of at most 0.00062.
Values may be sent and summed in bfloat16 or wider, within the bound.
No kernel may reach another device: no remote copies, remote signals or barrier semaphores. Data moves between devices by JAX's collectives and lax.ppermute only.
A program may use at most 64 MiB of HBM per device.

```python
import math
import jax
import jax.numpy as jnp
import numpy as np
from jax import lax

P_SIZE = 10
C = 8192
MAXB = 32
LINE_SLOTS = 128
LINES = 1024
NOBS = 131072


def draw_inv_band(key, part):
    first_key, second_key = jax.random.split(jax.random.fold_in(key, 17))
    coupling = jnp.clip(0.2 * jax.random.normal(first_key, (2 * MAXB - 1, C), jnp.float32), -1.0, 1.0)
    center = jnp.exp(jax.random.uniform(second_key, (C,), jnp.float32, jnp.log(0.5), jnp.log(2.0)))
    rows_at = jnp.arange(2 * MAXB - 1)[:, None]
    return jnp.where(rows_at == MAXB - 1, center[None, :], coupling).astype(jnp.bfloat16)


def observation_predictors(key):
    value_key = jax.random.fold_in(jax.random.fold_in(key, 101), 1)
    place = jnp.arange(NOBS, dtype=jnp.float32) / jnp.float32(NOBS)
    rising = 0.7 * jnp.exp(jnp.log(3.0) * place)
    level = rising
    values = jax.random.uniform(value_key, (P_SIZE, NOBS), jnp.float32, -1.0, 1.0)
    return values * level[None, :]


def draw_predictors(key, part):
    return observation_predictors(key).astype(jnp.bfloat16)


def draw_departures(key, part):
    pred = observation_predictors(key)
    coef_key, scale_key, noise_key = jax.random.split(jax.random.fold_in(key, 202), 3)
    scales = jnp.exp(jax.random.uniform(scale_key, (C,), jnp.float32, jnp.log(0.2), jnp.log(1.2)))
    coefs = 0.5 * jax.random.normal(coef_key, (C, P_SIZE), jnp.float32) * scales[:, None]
    block = 128
    coef_blocks = coefs.reshape(C // block, block, P_SIZE)

    def one_block(index):
        bias = jnp.dot(coef_blocks[index], pred, precision=lax.Precision.HIGHEST)
        block_key = jax.random.fold_in(noise_key, index)
        noise = 0.5 * jax.random.normal(block_key, (block, NOBS), jnp.float32)
        return jnp.clip(bias + noise, -8.0, 8.0).astype(jnp.bfloat16)
    blocks = lax.map(one_block, jnp.arange(C // block, dtype=jnp.int32))
    return blocks.reshape(C, NOBS)


def set_ends(result, stream_key, smallest, largest):
    shape = result.shape
    spot = [jax.random.randint(jax.random.fold_in(stream_key, axis), (), 0, shape[axis]) for axis in range(len(shape))]
    result = result.at[tuple(spot)].set(smallest)
    longest = shape.index(max(shape))
    spot[longest] = (spot[longest] + 1) % shape[longest]
    return result.at[tuple(spot)].set(largest)


def split_up(count, total, most, skew):
    weights = [(1 << 20) // math.isqrt(grade ** skew) + 1 for grade in range(2, count + 1)]
    surplus, holding = total - most - (count - 1), [1] * (count - 1)
    while surplus > 0:
        free = [i for i in range(count - 1) if holding[i] < most]
        mass, remaining = sum([weights[i] for i in free]), surplus
        for i in free:
            addition = min(most - holding[i], max(1, remaining * weights[i] // mass), surplus)
            holding[i] = holding[i] + addition
            surplus = surplus - addition
    return np.array([most] + holding)


def ragged(stream_key, number_of, total, most, skew):
    if number_of == 2:
        one = jax.random.randint(stream_key, (), max(1, total - most), min(most, total - 1) + 1)
        return jnp.stack([one, total - one])
    lengths = jnp.asarray(split_up(number_of, total, most, skew), jnp.int32)
    pairs = (number_of - 1) // 2
    source_of, receiver = lengths[1:1 + 2 * pairs:2], lengths[2:2 + 2 * pairs:2]
    room = jnp.minimum(source_of - 1, most - receiver)
    shifted = jax.random.randint(jax.random.fold_in(stream_key, 1), (pairs,), 0, 1 << 20) % (room + 1)
    lengths = lengths.at[1:1 + 2 * pairs:2].set(source_of - shifted).at[2:2 + 2 * pairs:2].set(receiver + shifted)
    return lengths[jax.random.permutation(jax.random.fold_in(stream_key, 2), number_of)]


def setup_inputs(seed: int = 0) -> dict:
    streams_of = jax.random.split(jax.random.key(seed), 6)
    departures = draw_departures(jax.random.fold_in(streams_of[5], 71), 0)
    predictors = draw_predictors(jax.random.fold_in(streams_of[5], 71), 0)
    inv_band = draw_inv_band(jax.random.fold_in(streams_of[5], 71), 0)
    band_id = jnp.searchsorted(jnp.cumsum(ragged(streams_of[3], C // 24, C, MAXB, 1)), jnp.arange(C), side="right").astype(jnp.int32)
    line_counts = set_ends(jax.random.randint(streams_of[4], (LINES,), 24, LINE_SLOTS + 1), jax.random.fold_in(streams_of[4], 1), 24, LINE_SLOTS).astype(jnp.int32)
    return {"departures": departures, "predictors": predictors, "inv_band": inv_band, "band_id": band_id, "line_counts": line_counts}


huber_edge = 1.0


def reference(departures, predictors, inv_band, band_id, line_counts):
    chans, nobs = departures.shape
    half = MAXB - 1
    tile = 128
    extent = tile + 2 * half
    slots = jnp.arange(nobs, dtype=jnp.int32)
    live = (slots % LINE_SLOTS < jnp.repeat(line_counts, LINE_SLOTS)).astype(jnp.float32)
    pred_wide = predictors.astype(jnp.float32).T
    pairs_t = (pred_wide[:, :, None] * pred_wide[:, None, :]).reshape(nobs, P_SIZE * P_SIZE).astype(jnp.bfloat16)
    pred_t = predictors.T

    def one_tile(index):
        first = index * tile
        start = jnp.clip(first - half, 0, chans - extent).astype(jnp.int32)
        rows_at = first + jnp.arange(tile, dtype=jnp.int32)
        cols_at = start + jnp.arange(extent, dtype=jnp.int32)
        offset = cols_at[None, :] - rows_at[:, None] + half
        keep = (offset >= 0) & (offset <= 2 * half) & (band_id[cols_at][None, :] == band_id[rows_at][:, None])
        values = inv_band[jnp.clip(offset, 0, 2 * half), rows_at[:, None]]
        matrix = jnp.where(keep, values, jnp.zeros_like(values))
        window = lax.dynamic_slice_in_dim(departures, start, extent, 0)
        weighted = jnp.dot(matrix, window, preferred_element_type=jnp.float32)
        ratio = live[None, :] * (huber_edge / jnp.maximum(jnp.abs(weighted), huber_edge))
        qc_weight = ratio.astype(jnp.bfloat16)
        scaled = (ratio * weighted).astype(jnp.bfloat16)
        gram_tile = jnp.dot(qc_weight, pairs_t, preferred_element_type=jnp.float32)
        rhs_tile = jnp.dot(scaled, pred_t, preferred_element_type=jnp.float32)
        return gram_tile, rhs_tile

    grams, rhss = lax.map(one_tile, jnp.arange(chans // tile, dtype=jnp.int32))
    gram = grams.reshape(chans, P_SIZE * P_SIZE).T / jnp.float32(nobs)
    rhs = rhss.reshape(chans, P_SIZE).T / jnp.float32(nobs)
    return gram, rhs
```

```python
import functools
import jax
import jax.numpy as jnp
from jax import lax
from jax.experimental import pallas as pl
from jax.experimental.pallas import tpu as pltpu
from jax.sharding import PartitionSpec as P

TILE = 128
HALO = 32
WIN = TILE + 2 * HALO
STEP = 256
OBS = 512
GROUP = 32
ROWS = 24

f32, bf16 = jnp.float32, jnp.bfloat16


def prepare_moments(pred, counts, w1_ref, w2_ref):
    count_pred, obs = pred.shape
    lines = counts.shape[0]
    slots = obs // lines
    pairs_n = count_pred * (count_pred + 1) // 2
    lane = lax.broadcasted_iota(jnp.int32, (1, slots), 1)
    column = lax.broadcasted_iota(jnp.int32, (slots, 128), 1)
    for line in range(lines):
        at = slice(line * slots, (line + 1) * slots)
        p = jnp.where(lane < counts[line], pred[:, at].astype(f32), 0.0)
        rows = [p[j : j + 1] * p[j:] for j in range(count_pred)] + [p]
        used = pairs_n + count_pred
        rows.append(jnp.zeros((128 - used, slots), f32))
        moments = jnp.concatenate(rows, axis=0).T
        w1_ref[at] = jnp.where(column < pairs_n, moments, 0.0).astype(bf16)
        w2_ref[at] = jnp.where(column >= pairs_n, moments, 0.0).astype(bf16)


def prepare_band(t, chan, inv_ref, ids_ref, band_ref):
    tiles = inv_ref.shape[1] // TILE
    total = ids_ref.shape[0]
    offsets = inv_ref.shape[0]
    at = chan * tiles + t
    own = ids_ref[pl.ds(at, 1)].astype(f32)
    before = ids_ref[pl.ds(jnp.maximum(at - 1, 0), 1)].astype(f32)
    after = ids_ref[pl.ds(jnp.minimum(at + 1, total - 1), 1)].astype(f32)
    before = jnp.where(at > 0, before, -1.0)
    after = jnp.where(at < total - 1, after, -1.0)
    near = jnp.concatenate(
        [before[:, TILE - HALO :], own, after[:, :HALO], jnp.full((1, 256 - WIN), -1.0, f32)],
        axis=1,
    )
    values = inv_ref[:, t * TILE : (t + 1) * TILE].astype(f32)
    stacked = jnp.concatenate([values, own, jnp.zeros((128 - offsets - 1, TILE), f32)], axis=0).T
    own_id = stacked[:, offsets : offsets + 1]
    column = lax.broadcasted_iota(jnp.int32, (TILE, 128), 1)
    wide = jnp.concatenate(
        [jnp.where(column < offsets, stacked, 0.0), jnp.zeros((TILE, 128), f32)], axis=1
    )
    skewed = pltpu.roll(wide, 1, 1, stride=1, stride_axis=0)
    band_ref[...] = jnp.where(own_id == near, skewed, 0.0).astype(bf16)


def weigh(window, matrix, qc_ref, scaled_ref, rows):
    for o in range(0, window.shape[1], OBS):
        at = slice(o, o + OBS)
        w = jnp.dot(matrix[:, :WIN], window[:, at], preferred_element_type=f32)
        ratio = 1.0 / jnp.maximum(jnp.abs(w), 1.0)
        qc_ref[rows, at] = ratio.astype(bf16)
        scaled_ref[rows, at] = jnp.clip(w, -1.0, 1.0).astype(bf16)


def reduce(first, qc_ref, scaled_ref, w1, w2, out_ref):
    lane = lax.broadcasted_iota(jnp.int32, (GROUP // 2, 128), 1)
    lane8 = lax.broadcasted_iota(jnp.int32, (8, 128), 1)
    total = jnp.dot(qc_ref[...], w1[...], preferred_element_type=f32)
    total += jnp.dot(scaled_ref[...], w2[...], preferred_element_type=f32)
    for g in range(STEP // GROUP):
        block = total[g * GROUP : (g + 1) * GROUP]
        low, high = block[: GROUP // 2], block[GROUP // 2 :]
        main = jnp.where(lane < 64, low, pltpu.roll(high, 64, 1))
        last = jnp.zeros((8, 128), f32)
        for v in range(GROUP // 8):
            moved = pltpu.roll(block[v * 8 : v * 8 + 8], 64 + v, 1)
            last = jnp.where(lane8 == v, moved, last)
        out_ref[first[g]] = jnp.concatenate([main, last], axis=0).astype(bf16)


def groups_of(*tiles):
    return [t * (TILE // GROUP) + g for t in tiles for g in range(TILE // GROUP)]


def inner_kernel(
    chan_ref, counts_hbm, pred_hbm, inv_hbm, ids_hbm, dep_hbm,
    out_ref, edge, edge_band, w1, w2,
    dep_all, band, qc, scaled, counts, pred, inv, ids, sems,
):
    own, obs = dep_hbm.shape
    tiles = own // TILE
    steps = tiles // 2 - 1
    chunks = own // STEP

    def copy(number, source, target):
        return pltpu.make_async_copy(source, target, sems.at[number])

    small = [
        copy(0, counts_hbm, counts),
        copy(1, pred_hbm, pred),
        copy(2, inv_hbm, inv),
        copy(3, ids_hbm, ids),
    ]
    rows = [pl.ds(s * STEP, STEP) for s in range(chunks)]
    large = [copy(4 + s, dep_hbm.at[rows[s]], dep_all.at[rows[s]]) for s in range(chunks)]
    kept = WIN - HALO
    ends = [
        copy(4 + chunks, dep_hbm.at[pl.ds(0, kept)], edge.at[0, pl.ds(HALO, kept)]),
        copy(5 + chunks, dep_hbm.at[pl.ds(own - kept, kept)], edge.at[1, pl.ds(0, kept)]),
    ]
    for c in small + large + ends:
        c.start()
    for c in small:
        c.wait()
    chan = chan_ref[0]
    prepare_moments(pred, counts, w1, w2)
    for t in range(tiles):
        if t == 0:
            prepare_band(t, chan, inv, ids, edge_band.at[0])
        elif t == tiles - 1:
            prepare_band(t, chan, inv, ids, edge_band.at[1])
        else:
            prepare_band(t, chan, inv, ids, band.at[t])
    arrived = 0
    for s in range(steps):
        needed = min(chunks, ((2 * s + 3) * TILE + HALO - 1) // STEP + 1)
        for c in large[arrived:needed]:
            c.wait()
        arrived = needed
        for half in range(2):
            t = 2 * s + 1 + half
            window = dep_all.at[pl.ds(t * TILE - HALO, WIN)]
            weigh(window, band.at[t], qc.at[s % 2], scaled.at[s % 2], pl.ds(half * TILE, TILE))
        if s > 0:
            p = s - 1
            reduce(groups_of(2 * p + 1, 2 * p + 2), qc.at[p % 2], scaled.at[p % 2], w1, w2, out_ref)
    p = steps - 1
    reduce(groups_of(2 * p + 1, 2 * p + 2), qc.at[p % 2], scaled.at[p % 2], w1, w2, out_ref)
    for c in large[arrived:] + ends:
        c.wait()


def edge_kernel(
    top_ref, bottom_ref, edge_band, w1, w2, parts_ref, edge_ref, out_ref, edge, qc, scaled
):
    tiles = parts_ref.shape[0] * GROUP // TILE
    edge[0, :HALO] = top_ref[...]
    edge[1, WIN - HALO :] = bottom_ref[...]
    for half in range(2):
        weigh(edge.at[half], edge_band.at[half], qc, scaled, pl.ds(half * TILE, TILE))
    reduce(groups_of(0, tiles - 1), qc, scaled, w1, w2, out_ref)


def border_kernel(dep_hbm, head_ref, tail_ref, sems):
    own = dep_hbm.shape[0]
    head = pltpu.make_async_copy(dep_hbm.at[pl.ds(0, HALO)], head_ref, sems.at[0])
    tail = pltpu.make_async_copy(dep_hbm.at[pl.ds(own - HALO, HALO)], tail_ref, sems.at[1])
    head.start()
    tail.start()
    head.wait()
    tail.wait()


def borders(departures):
    vmem = pl.BlockSpec(memory_space=pltpu.VMEM)
    rows = jax.ShapeDtypeStruct((HALO, departures.shape[1]), bf16)
    return pl.pallas_call(
        border_kernel,
        out_shape=(rows, rows),
        in_specs=[pl.BlockSpec(memory_space=pltpu.HBM)],
        out_specs=(vmem, vmem),
        scratch_shapes=[pltpu.SemaphoreType.DMA((2,))],
        compiler_params=pltpu.CompilerParams(vmem_limit_bytes=50 * 1024 * 1024),
        cost_estimate=pl.CostEstimate(flops=20_000_000_000, bytes_accessed=500_000, transcendentals=0),
        name="borders",
    )(departures)


def partial_sums(chan, counts, top, bottom, pred, inv_band, ids, departures):
    own, obs = departures.shape
    tiles = own // TILE
    vmem = pl.BlockSpec(memory_space=pltpu.VMEM)
    smem = pl.BlockSpec(memory_space=pltpu.SMEM)
    hbm = pl.BlockSpec(memory_space=pltpu.HBM)
    shape = jax.ShapeDtypeStruct
    parts_shape = shape((own // GROUP, ROWS, 128), bf16)
    edge_shape = shape((2, WIN, obs), bf16)
    parts, edge, edge_band, w1, w2 = pl.pallas_call(
        inner_kernel,
        out_shape=(
            parts_shape,
            edge_shape,
            shape((2, TILE, 256), bf16),
            shape((obs, 128), bf16),
            shape((obs, 128), bf16),
        ),
        in_specs=[smem, hbm, hbm, hbm, hbm, hbm],
        out_specs=(vmem,) * 5,
        scratch_shapes=[
            pltpu.VMEM((own, obs), bf16),
            pltpu.VMEM((tiles, TILE, 256), bf16),
            pltpu.VMEM((2, STEP, obs), bf16),
            pltpu.VMEM((2, STEP, obs), bf16),
            pltpu.SMEM(counts.shape, jnp.int32),
            pltpu.VMEM(pred.shape, bf16),
            pltpu.VMEM(inv_band.shape, bf16),
            pltpu.VMEM(ids.shape, jnp.int32),
            pltpu.SemaphoreType.DMA((6 + own // STEP,)),
        ],
        compiler_params=pltpu.CompilerParams(vmem_limit_bytes=50 * 1024 * 1024),
        cost_estimate=pl.CostEstimate(flops=12_000_000_000, bytes_accessed=9_000_000, transcendentals=0),
        name="inner",
    )(chan, counts, pred, inv_band, ids, departures)
    parts, _ = pl.pallas_call(
        edge_kernel,
        out_shape=(parts_shape, edge_shape),
        in_specs=[vmem] * 7,
        out_specs=(vmem, vmem),
        input_output_aliases={5: 0, 6: 1},
        scratch_shapes=[pltpu.VMEM((STEP, obs), bf16), pltpu.VMEM((STEP, obs), bf16)],
        compiler_params=pltpu.CompilerParams(vmem_limit_bytes=16 * 1024 * 1024),
        name="edge",
    )(top, bottom, edge_band, w1, w2, parts, edge)
    return parts


def finish_kernel(factor, place_ref, parts_ref, gram_ref, rhs_ref):
    count_pred = rhs_ref.shape[0]
    pairs_n = count_pred * (count_pred + 1) // 2
    half = GROUP // 2
    total = parts_ref[...].astype(f32).sum(axis=0) * factor
    main, last = total[:half], total[half:]
    lane = lax.broadcasted_iota(jnp.int32, (GROUP, 128), 1)
    joined = jnp.concatenate([main, pltpu.roll(main, 64, 1)], axis=0)
    ends = jnp.concatenate([pltpu.roll(last, 64 - v, 1) for v in range(GROUP // 8)], axis=0)
    joined = jnp.where(lane < 64, joined, ends)
    place = jnp.broadcast_to(place_ref[...], (GROUP, 128))
    gram = jnp.take_along_axis(joined, place, axis=1)
    gram_ref[...] = gram[:, : count_pred * count_pred]
    turned = jnp.concatenate([joined, jnp.zeros((128 - GROUP, 128), f32)], axis=0).T
    rhs_ref[...] = turned[pairs_n : pairs_n + count_pred, :GROUP]


def finish(parts, count_pred, factor):
    index = []
    for j in range(count_pred):
        for k in range(count_pred):
            a, b = min(j, k), max(j, k)
            index.append(a * count_pred - a * (a - 1) // 2 + b - a)
    index += [0] * (128 - len(index))
    vmem = pl.BlockSpec(memory_space=pltpu.VMEM)
    gram, rhs = pl.pallas_call(
        functools.partial(finish_kernel, factor),
        out_shape=(
            jax.ShapeDtypeStruct((GROUP, count_pred * count_pred), f32),
            jax.ShapeDtypeStruct((count_pred, GROUP), f32),
        ),
        in_specs=[vmem, vmem],
        out_specs=(vmem, vmem),
        compiler_params=pltpu.CompilerParams(vmem_limit_bytes=4 * 1024 * 1024),
        name="finish",
    )(jnp.array([index], jnp.int32), parts)
    return gram.T, rhs


def on_device(departures, predictors, inv_band, band_id, line_counts):
    own, obs = departures.shape
    count = lax.axis_size("chan")
    up = [(i, i + 1) for i in range(count - 1)]
    down = [(i + 1, i) for i in range(count - 1)]
    head, tail = borders(departures)
    top = lax.ppermute(tail, "chan", up)
    bottom = lax.ppermute(head, "chan", down)
    chan = lax.axis_index("chan").astype(jnp.int32).reshape(1)
    ids = band_id.reshape(-1, TILE)
    parts = partial_sums(chan, line_counts, top, bottom, predictors, inv_band, ids, departures)
    arrived = lax.all_to_all(parts, "obs", split_axis=0, concat_axis=0, tiled=True)
    return finish(arrived, predictors.shape[0], 1.0 / float(obs * lax.axis_size("obs")))


def solution(mesh):
    in_specs = (P("chan", "obs"), P(None, "obs"), P(None, "chan"), P(), P("obs"))
    out_specs = (P(None, ("chan", "obs")), P(None, ("chan", "obs")))
    return jax.shard_map(
        on_device, mesh=mesh, in_specs=in_specs, out_specs=out_specs, check_vma=False
    )
```

```python
import functools
import jax
import jax.numpy as jnp
from jax import lax
from jax.experimental import pallas as pl
from jax.experimental.pallas import tpu as pltpu
from jax.sharding import PartitionSpec as P

TILE = 128
HALO = 32
WIN = TILE + 2 * HALO
STEP = 256
PIECES = 16
WAITS = (4,)
AHEAD = 2
OBS = 512
GROUP = 32
ROWS = 24

f32, bf16 = jnp.float32, jnp.bfloat16


def prepare_moments(pred, counts, w1_ref, rows_ref):
    count_pred, obs = pred.shape
    lines = counts.shape[0]
    slots = obs // lines
    pairs_n = count_pred * (count_pred + 1) // 2
    offset = pairs_n % 8
    lane = lax.broadcasted_iota(jnp.int32, (1, slots), 1)
    for line in range(lines):
        at = slice(line * slots, (line + 1) * slots)
        p = jnp.where(lane < counts[line], pred[:, at].astype(f32), 0.0)
        rows = [p[j : j + 1] * p[j:] for j in range(count_pred)]
        rows.append(jnp.zeros((128 - pairs_n, slots), f32))
        w1_ref[at] = jnp.concatenate(rows, axis=0).T.astype(bf16)
        below = jnp.zeros((offset, slots), f32)
        above = jnp.zeros((32 - offset - count_pred, slots), f32)
        rows_ref[:, at] = jnp.concatenate([below, p, above], axis=0).astype(bf16)


def prepare_band(t, chan, inv_ref, ids_ref, band_ref):
    tiles = inv_ref.shape[1] // TILE
    total = ids_ref.shape[0]
    offsets = inv_ref.shape[0]
    at = chan * tiles + t
    own = ids_ref[pl.ds(at, 1)].astype(f32)
    before = ids_ref[pl.ds(jnp.maximum(at - 1, 0), 1)].astype(f32)
    after = ids_ref[pl.ds(jnp.minimum(at + 1, total - 1), 1)].astype(f32)
    before = jnp.where(at > 0, before, -1.0)
    after = jnp.where(at < total - 1, after, -1.0)
    near = jnp.concatenate(
        [before[:, TILE - HALO :], own, after[:, :HALO], jnp.full((1, 256 - WIN), -1.0, f32)],
        axis=1,
    )
    values = inv_ref[:, t * TILE : (t + 1) * TILE].astype(f32)
    stacked = jnp.concatenate([values, own, jnp.zeros((128 - offsets - 1, TILE), f32)], axis=0).T
    own_id = stacked[:, offsets : offsets + 1]
    column = lax.broadcasted_iota(jnp.int32, (TILE, 128), 1)
    wide = jnp.concatenate(
        [jnp.where(column < offsets, stacked, 0.0), jnp.zeros((TILE, 128), f32)], axis=1
    )
    skewed = pltpu.roll(wide, 1, 1, stride=1, stride_axis=0)
    band_ref[...] = jnp.where(own_id == near, skewed, 0.0).astype(bf16)


def weigh(window, matrix, qc_ref, scaled_ref, rows):
    for o in range(0, window.shape[1], OBS):
        at = slice(o, o + OBS)
        w = jnp.dot(matrix[:, :WIN], window[:, at], preferred_element_type=f32)
        ratio = 1.0 / jnp.maximum(jnp.abs(w), 1.0)
        qc_ref[rows, at] = ratio.astype(bf16)
        scaled_ref[rows, at] = jnp.clip(w, -1.0, 1.0).astype(bf16)


def reduce(first, qc_ref, scaled_ref, w1, w2, out_ref):
    lane = lax.broadcasted_iota(jnp.int32, (GROUP // 2, 128), 1)
    lane8 = lax.broadcasted_iota(jnp.int32, (8, 128), 1)
    total = jnp.dot(qc_ref[...], w1[...], preferred_element_type=f32)
    obs = scaled_ref.shape[1]
    below = jnp.zeros((48, STEP), f32)
    for at in (slice(0, obs // 2), slice(obs // 2, obs)):
        turned = lax.dot_general(
            w2[:, at], scaled_ref[:, at], (((1,), (1,)), ((), ())), preferred_element_type=f32
        )
        total += jnp.concatenate([below, turned, below], axis=0).T
    for g in range(STEP // GROUP):
        block = total[g * GROUP : (g + 1) * GROUP]
        low, high = block[: GROUP // 2], block[GROUP // 2 :]
        main = jnp.where(lane < 64, low, pltpu.roll(high, 64, 1))
        last = jnp.zeros((8, 128), f32)
        for v in range(GROUP // 8):
            moved = pltpu.roll(block[v * 8 : v * 8 + 8], 64 + v, 1)
            last = jnp.where(lane8 == v, moved, last)
        out_ref[first[g]] = jnp.concatenate([main, last], axis=0).astype(bf16)


def groups_of(*tiles):
    return [t * (TILE // GROUP) + g for t in tiles for g in range(TILE // GROUP)]


def inner_kernel(
    chan_ref, counts_hbm, pred_hbm, inv_hbm, ids_hbm, dep_hbm,
    out_ref, edge, edge_band, w1, w2,
    dep_all, band, qc, scaled, counts, pred, inv, ids, sems,
):
    own, obs = dep_hbm.shape
    tiles = own // TILE
    steps = tiles // 2 - 1

    def copy(number, source, target):
        return pltpu.make_async_copy(source, target, sems.at[number])

    small = [
        copy(0, counts_hbm, counts),
        copy(1, pred_hbm, pred),
        copy(2, inv_hbm, inv),
        copy(3, ids_hbm, ids),
    ]
    cuts = [(n * own // PIECES) for n in range(PIECES + 1)]
    rows = [pl.ds(a, b - a) for a, b in zip(cuts, cuts[1:])]
    large = [copy(4 + n, dep_hbm.at[r], dep_all.at[r]) for n, r in enumerate(rows)]
    kept = WIN - HALO
    ends = [
        copy(4 + PIECES, dep_hbm.at[pl.ds(0, kept)], edge.at[0, pl.ds(HALO, kept)]),
        copy(5 + PIECES, dep_hbm.at[pl.ds(own - kept, kept)], edge.at[1, pl.ds(0, kept)]),
    ]
    for c in small + large + ends:
        c.start()
    for c in small:
        c.wait()
    chan = chan_ref[0]
    prepare_moments(pred, counts, w1, w2)

    def prepare(t):
        if t == 0:
            prepare_band(t, chan, inv, ids, edge_band.at[0])
        elif t == tiles - 1:
            prepare_band(t, chan, inv, ids, edge_band.at[1])
        else:
            prepare_band(t, chan, inv, ids, band.at[t])

    def weigh_step(s):
        for half in range(2):
            t = 2 * s + 1 + half
            window = dep_all.at[pl.ds(t * TILE - HALO, WIN)]
            weigh(window, band.at[t], qc.at[s % 2], scaled.at[s % 2], pl.ds(half * TILE, TILE))

    def reduce_step(s):
        groups = groups_of(2 * s + 1, 2 * s + 2)
        reduce(groups, qc.at[s % 2], scaled.at[s % 2], w1, w2, out_ref)

    order = [(2 * s + 1, 2 * s + 2) for s in range(steps)] + [(0, tiles - 1)]
    for pair in order[:AHEAD]:
        prepare(pair[0])
        prepare(pair[1])
    arrived = 0
    for s in range(steps):
        if s > 0:
            reduce_step(s - 1)
        needed = next(n for n in range(PIECES + 1) if cuts[n] >= (2 * s + 3) * TILE + HALO)
        if needed > arrived:
            until = next((n for n in WAITS if n >= needed), PIECES)
            for c in large[arrived:until]:
                c.wait()
            arrived = until
        weigh_step(s)
        for pair in order[s + AHEAD : s + AHEAD + 1]:
            prepare(pair[0])
            prepare(pair[1])
    reduce_step(steps - 1)
    for c in large[arrived:] + ends:
        c.wait()


def edge_kernel(
    top_ref, bottom_ref, edge_band, w1, w2, parts_ref, edge_ref, out_ref, edge, qc, scaled
):
    tiles = parts_ref.shape[0] * GROUP // TILE
    edge[0, :HALO] = top_ref[...]
    edge[1, WIN - HALO :] = bottom_ref[...]
    for half in range(2):
        weigh(edge.at[half], edge_band.at[half], qc, scaled, pl.ds(half * TILE, TILE))
    reduce(groups_of(0, tiles - 1), qc, scaled, w1, w2, out_ref)


def border_kernel(dep_hbm, head_ref, tail_ref, sems):
    own = dep_hbm.shape[0]
    head = pltpu.make_async_copy(dep_hbm.at[pl.ds(0, HALO)], head_ref, sems.at[0])
    tail = pltpu.make_async_copy(dep_hbm.at[pl.ds(own - HALO, HALO)], tail_ref, sems.at[1])
    head.start()
    tail.start()
    head.wait()
    tail.wait()


def borders(departures):
    vmem = pl.BlockSpec(memory_space=pltpu.VMEM)
    rows = jax.ShapeDtypeStruct((HALO, departures.shape[1]), bf16)
    return pl.pallas_call(
        border_kernel,
        out_shape=(rows, rows),
        in_specs=[pl.BlockSpec(memory_space=pltpu.HBM)],
        out_specs=(vmem, vmem),
        scratch_shapes=[pltpu.SemaphoreType.DMA((2,))],
        compiler_params=pltpu.CompilerParams(vmem_limit_bytes=50 * 1024 * 1024),
        cost_estimate=pl.CostEstimate(flops=20_000_000_000, bytes_accessed=500_000, transcendentals=0),
        name="borders",
    )(departures)


def partial_sums(chan, counts, top, bottom, pred, inv_band, ids, departures):
    own, obs = departures.shape
    tiles = own // TILE
    vmem = pl.BlockSpec(memory_space=pltpu.VMEM)
    smem = pl.BlockSpec(memory_space=pltpu.SMEM)
    hbm = pl.BlockSpec(memory_space=pltpu.HBM)
    shape = jax.ShapeDtypeStruct
    parts_shape = shape((own // GROUP, ROWS, 128), bf16)
    edge_shape = shape((2, WIN, obs), bf16)
    parts, edge, edge_band, w1, w2 = pl.pallas_call(
        inner_kernel,
        out_shape=(
            parts_shape,
            edge_shape,
            shape((2, TILE, 256), bf16),
            shape((obs, 128), bf16),
            shape((32, obs), bf16),
        ),
        in_specs=[smem, hbm, hbm, hbm, hbm, hbm],
        out_specs=(vmem,) * 5,
        scratch_shapes=[
            pltpu.VMEM((own, obs), bf16),
            pltpu.VMEM((tiles, TILE, 256), bf16),
            pltpu.VMEM((2, STEP, obs), bf16),
            pltpu.VMEM((2, STEP, obs), bf16),
            pltpu.SMEM(counts.shape, jnp.int32),
            pltpu.VMEM(pred.shape, bf16),
            pltpu.VMEM(inv_band.shape, bf16),
            pltpu.VMEM(ids.shape, jnp.int32),
            pltpu.SemaphoreType.DMA((6 + PIECES,)),
        ],
        compiler_params=pltpu.CompilerParams(vmem_limit_bytes=50 * 1024 * 1024),
        cost_estimate=pl.CostEstimate(flops=12_000_000_000, bytes_accessed=9_000_000, transcendentals=0),
        name="inner",
    )(chan, counts, pred, inv_band, ids, departures)
    parts, _ = pl.pallas_call(
        edge_kernel,
        out_shape=(parts_shape, edge_shape),
        in_specs=[vmem] * 7,
        out_specs=(vmem, vmem),
        input_output_aliases={5: 0, 6: 1},
        scratch_shapes=[pltpu.VMEM((STEP, obs), bf16), pltpu.VMEM((STEP, obs), bf16)],
        compiler_params=pltpu.CompilerParams(vmem_limit_bytes=16 * 1024 * 1024),
        name="edge",
    )(top, bottom, edge_band, w1, w2, parts, edge)
    return parts


def finish_kernel(factor, place_ref, parts_ref, gram_ref, rhs_ref):
    count_pred = rhs_ref.shape[0]
    pairs_n = count_pred * (count_pred + 1) // 2
    half = GROUP // 2
    total = parts_ref[...].astype(f32).sum(axis=0) * factor
    main, last = total[:half], total[half:]
    lane = lax.broadcasted_iota(jnp.int32, (GROUP, 128), 1)
    joined = jnp.concatenate([main, pltpu.roll(main, 64, 1)], axis=0)
    ends = jnp.concatenate([pltpu.roll(last, 64 - v, 1) for v in range(GROUP // 8)], axis=0)
    joined = jnp.where(lane < 64, joined, ends)
    place = jnp.broadcast_to(place_ref[...], (GROUP, 128))
    gram = jnp.take_along_axis(joined, place, axis=1)
    gram_ref[...] = gram[:, : count_pred * count_pred]
    turned = jnp.concatenate([joined, jnp.zeros((128 - GROUP, 128), f32)], axis=0).T
    rhs_ref[...] = turned[pairs_n : pairs_n + count_pred, :GROUP]


def finish(parts, count_pred, factor):
    index = []
    for j in range(count_pred):
        for k in range(count_pred):
            a, b = min(j, k), max(j, k)
            index.append(a * count_pred - a * (a - 1) // 2 + b - a)
    index += [0] * (128 - len(index))
    vmem = pl.BlockSpec(memory_space=pltpu.VMEM)
    gram, rhs = pl.pallas_call(
        functools.partial(finish_kernel, factor),
        out_shape=(
            jax.ShapeDtypeStruct((GROUP, count_pred * count_pred), f32),
            jax.ShapeDtypeStruct((count_pred, GROUP), f32),
        ),
        in_specs=[vmem, vmem],
        out_specs=(vmem, vmem),
        compiler_params=pltpu.CompilerParams(vmem_limit_bytes=4 * 1024 * 1024),
        name="finish",
    )(jnp.array([index], jnp.int32), parts)
    return gram.T, rhs


def on_device(departures, predictors, inv_band, band_id, line_counts):
    own, obs = departures.shape
    count = lax.axis_size("chan")
    up = [(i, i + 1) for i in range(count - 1)]
    down = [(i + 1, i) for i in range(count - 1)]
    head, tail = borders(departures)
    top = lax.ppermute(tail, "chan", up)
    bottom = lax.ppermute(head, "chan", down)
    chan = lax.axis_index("chan").astype(jnp.int32).reshape(1)
    ids = band_id.reshape(-1, TILE)
    parts = partial_sums(chan, line_counts, top, bottom, predictors, inv_band, ids, departures)
    arrived = lax.all_to_all(parts, "obs", split_axis=0, concat_axis=0, tiled=True)
    return finish(arrived, predictors.shape[0], 1.0 / float(obs * lax.axis_size("obs")))


def solution(mesh):
    in_specs = (P("chan", "obs"), P(None, "obs"), P(None, "chan"), P(), P("obs"))
    out_specs = (P(None, ("chan", "obs")), P(None, ("chan", "obs")))
    return jax.shard_map(
        on_device, mesh=mesh, in_specs=in_specs, out_specs=out_specs, check_vma=False
    )
```

```python
import functools
import jax
import jax.numpy as jnp
from jax import lax
from jax.experimental import pallas as pl
from jax.experimental.pallas import tpu as pltpu
from jax.sharding import PartitionSpec as P

TILE = 128
HALO = 32
WIN = TILE + 2 * HALO
STEP = 256
PIECES = 8
WAITS = (2, 4)
AHEAD = 2
OBS = 512
GROUP = 32
ROWS = 24

f32, bf16 = jnp.float32, jnp.bfloat16


def prepare_moments(pred, counts, w1_ref, rows_ref):
    count_pred, obs = pred.shape
    lines = counts.shape[0]
    slots = obs // lines
    pairs_n = count_pred * (count_pred + 1) // 2
    offset = pairs_n % 8
    lane = lax.broadcasted_iota(jnp.int32, (1, slots), 1)
    for line in range(lines):
        at = slice(line * slots, (line + 1) * slots)
        p = jnp.where(lane < counts[line], pred[:, at].astype(f32), 0.0)
        rows = [p[j : j + 1] * p[j:] for j in range(count_pred)]
        rows.append(jnp.zeros((128 - pairs_n, slots), f32))
        w1_ref[at] = jnp.concatenate(rows, axis=0).T.astype(bf16)
        below = jnp.zeros((offset, slots), f32)
        above = jnp.zeros((32 - offset - count_pred, slots), f32)
        rows_ref[:, at] = jnp.concatenate([below, p, above], axis=0).astype(bf16)


def prepare_band(t, chan, inv_ref, ids_ref, band_ref):
    tiles = inv_ref.shape[1] // TILE
    total = ids_ref.shape[0]
    offsets = inv_ref.shape[0]
    at = chan * tiles + t
    own = ids_ref[pl.ds(at, 1)].astype(f32)
    before = ids_ref[pl.ds(jnp.maximum(at - 1, 0), 1)].astype(f32)
    after = ids_ref[pl.ds(jnp.minimum(at + 1, total - 1), 1)].astype(f32)
    before = jnp.where(at > 0, before, -1.0)
    after = jnp.where(at < total - 1, after, -1.0)
    near = jnp.concatenate(
        [before[:, TILE - HALO :], own, after[:, :HALO], jnp.full((1, 256 - WIN), -1.0, f32)],
        axis=1,
    )
    values = inv_ref[:, t * TILE : (t + 1) * TILE].astype(f32)
    stacked = jnp.concatenate([values, own, jnp.zeros((128 - offsets - 1, TILE), f32)], axis=0).T
    own_id = stacked[:, offsets : offsets + 1]
    column = lax.broadcasted_iota(jnp.int32, (TILE, 128), 1)
    wide = jnp.concatenate(
        [jnp.where(column < offsets, stacked, 0.0), jnp.zeros((TILE, 128), f32)], axis=1
    )
    skewed = pltpu.roll(wide, 1, 1, stride=1, stride_axis=0)
    band_ref[...] = jnp.where(own_id == near, skewed, 0.0).astype(bf16)


def weigh(window, matrix, qc_ref, scaled_ref, rows):
    for o in range(0, window.shape[1], OBS):
        at = slice(o, o + OBS)
        w = jnp.dot(matrix[:, :WIN], window[:, at], preferred_element_type=f32)
        ratio = 1.0 / jnp.maximum(jnp.abs(w), 1.0)
        qc_ref[rows, at] = ratio.astype(bf16)
        scaled_ref[rows, at] = jnp.clip(w, -1.0, 1.0).astype(bf16)


def reduce(first, qc_ref, scaled_ref, w1, w2, out_ref):
    lane = lax.broadcasted_iota(jnp.int32, (GROUP // 2, 128), 1)
    lane8 = lax.broadcasted_iota(jnp.int32, (8, 128), 1)
    total = jnp.dot(qc_ref[...], w1[...], preferred_element_type=f32)
    obs = scaled_ref.shape[1]
    below = jnp.zeros((48, STEP), f32)
    for at in (slice(0, obs // 2), slice(obs // 2, obs)):
        turned = lax.dot_general(
            w2[:, at], scaled_ref[:, at], (((1,), (1,)), ((), ())), preferred_element_type=f32
        )
        total += jnp.concatenate([below, turned, below], axis=0).T
    for g in range(STEP // GROUP):
        block = total[g * GROUP : (g + 1) * GROUP]
        low, high = block[: GROUP // 2], block[GROUP // 2 :]
        main = jnp.where(lane < 64, low, pltpu.roll(high, 64, 1))
        last = jnp.zeros((8, 128), f32)
        for v in range(GROUP // 8):
            moved = pltpu.roll(block[v * 8 : v * 8 + 8], 64 + v, 1)
            last = jnp.where(lane8 == v, moved, last)
        out_ref[first[g]] = jnp.concatenate([main, last], axis=0).astype(bf16)


def groups_of(*tiles):
    return [t * (TILE // GROUP) + g for t in tiles for g in range(TILE // GROUP)]


def inner_kernel(
    counts_hbm, pred, inv, ids, dep_hbm,
    out_ref, edge, edge_band, w1, w2,
    dep_all, band, qc, scaled, counts, sems,
):
    own, obs = dep_hbm.shape
    tiles = own // TILE
    steps = tiles // 2 - 1

    def copy(number, source, target):
        return pltpu.make_async_copy(source, target, sems.at[number])

    small = [copy(0, counts_hbm, counts)]
    cuts = [(n * own // PIECES) for n in range(PIECES + 1)]
    rows = [pl.ds(a, b - a) for a, b in zip(cuts, cuts[1:])]
    large = [copy(1 + n, dep_hbm.at[r], dep_all.at[r]) for n, r in enumerate(rows)]
    kept = WIN - HALO
    ends = [
        copy(1 + PIECES, dep_hbm.at[pl.ds(0, kept)], edge.at[0, pl.ds(HALO, kept)]),
        copy(2 + PIECES, dep_hbm.at[pl.ds(own - kept, kept)], edge.at[1, pl.ds(0, kept)]),
    ]
    for c in small + large + ends:
        c.start()
    for c in small:
        c.wait()
    chan = lax.axis_index("chan").astype(jnp.int32)
    prepare_moments(pred, counts, w1, w2)

    def prepare(t):
        if t == 0:
            prepare_band(t, chan, inv, ids, edge_band.at[0])
        elif t == tiles - 1:
            prepare_band(t, chan, inv, ids, edge_band.at[1])
        else:
            prepare_band(t, chan, inv, ids, band.at[t])

    def weigh_step(s):
        for half in range(2):
            t = 2 * s + 1 + half
            window = dep_all.at[pl.ds(t * TILE - HALO, WIN)]
            weigh(window, band.at[t], qc.at[s % 2], scaled.at[s % 2], pl.ds(half * TILE, TILE))

    def reduce_step(s):
        groups = groups_of(2 * s + 1, 2 * s + 2)
        reduce(groups, qc.at[s % 2], scaled.at[s % 2], w1, w2, out_ref)

    order = [(2 * s + 1, 2 * s + 2) for s in range(steps)] + [(0, tiles - 1)]
    for pair in order[:AHEAD]:
        prepare(pair[0])
        prepare(pair[1])
    arrived = 0
    for s in range(steps):
        if s > 0:
            reduce_step(s - 1)
        needed = next(n for n in range(PIECES + 1) if cuts[n] >= (2 * s + 3) * TILE + HALO)
        if needed > arrived:
            until = next((n for n in WAITS if n >= needed), PIECES)
            for c in large[arrived:until]:
                c.wait()
            arrived = until
        weigh_step(s)
        for pair in order[s + AHEAD : s + AHEAD + 1]:
            prepare(pair[0])
            prepare(pair[1])
    reduce_step(steps - 1)
    for c in large[arrived:] + ends:
        c.wait()


def edge_kernel(
    top_ref, bottom_ref, edge_band, w1, w2, parts_ref, edge_ref, out_ref, edge, qc, scaled
):
    tiles = parts_ref.shape[0] * GROUP // TILE
    edge[0, :HALO] = top_ref[...]
    edge[1, WIN - HALO :] = bottom_ref[...]
    for half in range(2):
        weigh(edge.at[half], edge_band.at[half], qc, scaled, pl.ds(half * TILE, TILE))
    reduce(groups_of(0, tiles - 1), qc, scaled, w1, w2, out_ref)


def border_kernel(dep_hbm, head_ref, tail_ref, sems):
    own = dep_hbm.shape[0]
    head = pltpu.make_async_copy(dep_hbm.at[pl.ds(0, HALO)], head_ref, sems.at[0])
    tail = pltpu.make_async_copy(dep_hbm.at[pl.ds(own - HALO, HALO)], tail_ref, sems.at[1])
    head.start()
    tail.start()
    head.wait()
    tail.wait()


def borders(departures):
    vmem = pl.BlockSpec(memory_space=pltpu.VMEM)
    rows = jax.ShapeDtypeStruct((HALO, departures.shape[1]), bf16)
    return pl.pallas_call(
        border_kernel,
        out_shape=(rows, rows),
        in_specs=[pl.BlockSpec(memory_space=pltpu.HBM)],
        out_specs=(vmem, vmem),
        scratch_shapes=[pltpu.SemaphoreType.DMA((2,))],
        compiler_params=pltpu.CompilerParams(vmem_limit_bytes=50 * 1024 * 1024),
        cost_estimate=pl.CostEstimate(flops=20_000_000_000, bytes_accessed=500_000, transcendentals=0),
        name="borders",
    )(departures)


def partial_sums(counts, top, bottom, pred, inv_band, ids, departures):
    own, obs = departures.shape
    tiles = own // TILE
    vmem = pl.BlockSpec(memory_space=pltpu.VMEM)
    hbm = pl.BlockSpec(memory_space=pltpu.HBM)
    shape = jax.ShapeDtypeStruct
    parts_shape = shape((own // GROUP, ROWS, 128), bf16)
    edge_shape = shape((2, WIN, obs), bf16)
    parts, edge, edge_band, w1, w2 = pl.pallas_call(
        inner_kernel,
        out_shape=(
            parts_shape,
            edge_shape,
            shape((2, TILE, 256), bf16),
            shape((obs, 128), bf16),
            shape((32, obs), bf16),
        ),
        in_specs=[hbm, vmem, vmem, vmem, hbm],
        out_specs=(vmem,) * 5,
        scratch_shapes=[
            pltpu.VMEM((own, obs), bf16),
            pltpu.VMEM((tiles, TILE, 256), bf16),
            pltpu.VMEM((2, STEP, obs), bf16),
            pltpu.VMEM((2, STEP, obs), bf16),
            pltpu.SMEM(counts.shape, jnp.int32),
            pltpu.SemaphoreType.DMA((3 + PIECES,)),
        ],
        compiler_params=pltpu.CompilerParams(vmem_limit_bytes=50 * 1024 * 1024),
        cost_estimate=pl.CostEstimate(flops=12_000_000_000, bytes_accessed=9_000_000, transcendentals=0),
        name="inner",
    )(counts, pred, inv_band, ids, departures)
    parts, _ = pl.pallas_call(
        edge_kernel,
        out_shape=(parts_shape, edge_shape),
        in_specs=[vmem] * 7,
        out_specs=(vmem, vmem),
        input_output_aliases={5: 0, 6: 1},
        scratch_shapes=[pltpu.VMEM((STEP, obs), bf16), pltpu.VMEM((STEP, obs), bf16)],
        compiler_params=pltpu.CompilerParams(vmem_limit_bytes=16 * 1024 * 1024),
        name="edge",
    )(top, bottom, edge_band, w1, w2, parts, edge)
    return parts


def finish_kernel(factor, place_ref, parts_ref, gram_ref, rhs_ref):
    count_pred = rhs_ref.shape[0]
    pairs_n = count_pred * (count_pred + 1) // 2
    half = GROUP // 2
    total = parts_ref[...].astype(f32).sum(axis=0) * factor
    main, last = total[:half], total[half:]
    lane = lax.broadcasted_iota(jnp.int32, (GROUP, 128), 1)
    joined = jnp.concatenate([main, pltpu.roll(main, 64, 1)], axis=0)
    ends = jnp.concatenate([pltpu.roll(last, 64 - v, 1) for v in range(GROUP // 8)], axis=0)
    joined = jnp.where(lane < 64, joined, ends)
    place = jnp.broadcast_to(place_ref[...], (GROUP, 128))
    gram = jnp.take_along_axis(joined, place, axis=1)
    gram_ref[...] = gram[:, : count_pred * count_pred]
    turned = jnp.concatenate([joined, jnp.zeros((128 - GROUP, 128), f32)], axis=0).T
    rhs_ref[...] = turned[pairs_n : pairs_n + count_pred, :GROUP]


def finish(parts, count_pred, factor):
    index = []
    for j in range(count_pred):
        for k in range(count_pred):
            a, b = min(j, k), max(j, k)
            index.append(a * count_pred - a * (a - 1) // 2 + b - a)
    index += [0] * (128 - len(index))
    vmem = pl.BlockSpec(memory_space=pltpu.VMEM)
    gram, rhs = pl.pallas_call(
        functools.partial(finish_kernel, factor),
        out_shape=(
            jax.ShapeDtypeStruct((GROUP, count_pred * count_pred), f32),
            jax.ShapeDtypeStruct((count_pred, GROUP), f32),
        ),
        in_specs=[vmem, vmem],
        out_specs=(vmem, vmem),
        compiler_params=pltpu.CompilerParams(vmem_limit_bytes=4 * 1024 * 1024),
        name="finish",
    )(jnp.array([index], jnp.int32), parts)
    return gram.T, rhs


def on_device(departures, predictors, inv_band, band_id, line_counts):
    own, obs = departures.shape
    count = lax.axis_size("chan")
    up = [(i, i + 1) for i in range(count - 1)]
    down = [(i + 1, i) for i in range(count - 1)]
    head, tail = borders(departures)
    top = lax.ppermute(tail, "chan", up)
    bottom = lax.ppermute(head, "chan", down)
    ids = band_id.reshape(-1, TILE)
    parts = partial_sums(line_counts, top, bottom, predictors, inv_band, ids, departures)
    arrived = lax.all_to_all(parts, "obs", split_axis=0, concat_axis=0, tiled=True)
    return finish(arrived, predictors.shape[0], 1.0 / float(obs * lax.axis_size("obs")))


def solution(mesh):
    in_specs = (P("chan", "obs"), P(None, "obs"), P(None, "chan"), P(), P("obs"))
    out_specs = (P(None, ("chan", "obs")), P(None, ("chan", "obs")))
    return jax.shard_map(
        on_device, mesh=mesh, in_specs=in_specs, out_specs=out_specs, check_vma=False
    )
```
